32 devices in a mesh: dp: 1 (over z), vp: 32 (over y, x, core).
Axes of the slice: x: 4, y: 4, z: 1, core: 2. Of those that a mesh axis runs over, the one named last changes fastest.
The devices are a block of a 4x4x8 slice.
Arguments:
- hidden: bfloat16 [8192, 2560], P(('dp', 'vp'))
- labels: int32 [8192], P(('dp', 'vp'))
- loss_weight: float32 [8192], P(('dp', 'vp'))
- norm_gain: float32 [2560], replicated
- w_unembed: bfloat16 [2560, 51328], P(None, 'vp')
Outputs:
- output 1: float32 [1], P('dp')
- output 2: bfloat16 [8192, 2560], P(('dp', 'vp'))
- output 3: float32 [2560, 51328], P('dp', 'vp')
- output 4: float32 [2560], P('dp')
All inputs are finite; a program needn't handle non-finite values.
Results may differ from the reference program's by a relative error of at most 0.001.
Values are sent between devices in bfloat16 or wider.
A program may use at most 768 MiB of HBM per device.

```python
import jax
import jax.numpy as jnp
from jax import lax

D = 2560
V = 51200
PAD_COLS = 128
TOK_DEV = 256
GROUP_SIZE = 32
VOCAB_PAD = V + PAD_COLS
TOKENS = TOK_DEV * GROUP_SIZE
LOW_IDS = V // 64
NORM_EPS = 1e-5


def setup_inputs(seed: int = 0, part: int = 0) -> dict:
    base_key = jax.random.key(seed)
    shared_key, parts_key = jax.random.split(base_key)
    part_key = jax.random.fold_in(parts_key, part)
    key_hid, key_pick, key_low, key_any, key_pad, key_wt = jax.random.split(part_key, 6)
    key_gain, key_unemb = jax.random.split(shared_key)
    hidden = jax.random.normal(key_hid, (TOKENS, D), jnp.float32).astype(jnp.bfloat16)
    tok_ids = jnp.arange(TOKENS)
    pick_low = jax.random.randint(key_pick, (TOKENS,), 0, 2)
    low_ids = jax.random.randint(key_low, (TOKENS,), 0, LOW_IDS)
    any_ids = jax.random.randint(key_any, (TOKENS,), 0, V)
    labels = jnp.where(pick_low == 0, low_ids, any_ids)
    labels = jnp.where(tok_ids == TOKENS - 1, V - 1, labels).astype(jnp.int32)
    pad_draw = jax.random.randint(key_pad, (TOKENS,), 0, 8)
    is_pad = (pad_draw == 0) & (tok_ids > 0)
    weight_val = jax.random.uniform(key_wt, (TOKENS,), jnp.float32, 0.25, 1.75)
    loss_weight = jnp.where(is_pad, 0.0, weight_val).astype(jnp.float32)
    norm_gain = 1.0 + 0.25 * jax.random.normal(key_gain, (D,), jnp.float32)
    w_unembed = (jax.random.normal(key_unemb, (D, VOCAB_PAD), jnp.float32) * (2.0 * D ** -0.5)).astype(jnp.bfloat16)
    return {"hidden": hidden, "labels": labels, "loss_weight": loss_weight, "norm_gain": norm_gain, "w_unembed": w_unembed}


def reference(hidden, labels, loss_weight, norm_gain, w_unembed):
    x_float = hidden.astype(jnp.float32)
    inv_rms = lax.rsqrt(jnp.mean(x_float * x_float, axis=-1, keepdims=True) + NORM_EPS)
    x_norm = x_float * inv_rms
    normed = (x_norm * norm_gain).astype(jnp.bfloat16)
    tok_scale = loss_weight / jnp.sum(loss_weight)
    col_ids = jnp.arange(VOCAB_PAD)[None, :]

    def block_step(d_unembed, block_in):
        normed_blk, label_blk, scale_blk = block_in
        logits = jnp.dot(normed_blk, w_unembed, preferred_element_type=jnp.float32)
        logits = jnp.where(col_ids < V, logits, -jnp.inf)
        is_target = col_ids == label_blk[:, None]
        row_max = jnp.max(logits, axis=1, keepdims=True)
        log_norm = row_max + jnp.log(jnp.sum(jnp.exp(logits - row_max), axis=1, keepdims=True))
        target = jnp.sum(jnp.where(is_target, logits, 0.0), axis=1, keepdims=True)
        tok_loss = (log_norm - target)[:, 0] * scale_blk
        d_logits = ((jnp.exp(logits - log_norm) - jnp.where(is_target, 1.0, 0.0)) * scale_blk[:, None]).astype(jnp.bfloat16)
        d_unembed = d_unembed + jnp.dot(normed_blk.T, d_logits, preferred_element_type=jnp.float32)
        d_normed = jnp.dot(d_logits, w_unembed.T, preferred_element_type=jnp.float32)
        return d_unembed, (tok_loss, d_normed)

    blocks = (normed.reshape(GROUP_SIZE, TOK_DEV, D), labels.reshape(GROUP_SIZE, TOK_DEV), tok_scale.reshape(GROUP_SIZE, TOK_DEV))
    d_unembed, (tok_loss, d_normed) = lax.scan(block_step, jnp.zeros((D, VOCAB_PAD), jnp.float32), blocks)
    d_normed = d_normed.reshape(TOKENS, D)
    mean_loss = jnp.sum(tok_loss).reshape(1)
    grad_hat = d_normed * norm_gain
    d_input = inv_rms * (grad_hat - x_norm * jnp.mean(grad_hat * x_norm, axis=-1, keepdims=True))
    d_norm_gain = jnp.sum(d_normed * x_norm, axis=0)
    return mean_loss, d_input.astype(jnp.bfloat16), d_unembed, d_norm_gain
```

```python
import functools
import math

import jax
import jax.numpy as jnp
from jax import lax
from jax.experimental import pallas as pl
from jax.experimental.pallas import tpu as pltpu
from jax.sharding import PartitionSpec as P

NORM_EPS = 1e-5
PAD_COLS = 128
LANE = 128
TILE = 256
TOKENS = 512
EIGHTHS = (3, 5)
LOWEST = float(jnp.finfo(jnp.float32).min)


def rows_to_columns(rows):
    return jnp.concatenate([rows] * (LANE // 8), 0).T


def logits_kernel(info_ref, ids_ref, a_ref, w_ref, z_ref, stat_ref, top_ref, sum_ref, hit_ref):
    label = rows_to_columns(info_ref[...])[:, 0:1]
    top_ref[...] = jnp.full_like(top_ref, LOWEST)
    sum_ref[...] = jnp.zeros_like(sum_ref)
    hit_ref[...] = jnp.zeros_like(hit_ref)
    tiles = w_ref.shape[0] // TILE

    def step(j, carry):
        cols = pl.ds(pl.multiple_of(j * TILE, TILE), TILE)
        ids = ids_ref[:, cols]
        z = lax.dot_general(a_ref[...], w_ref[cols, :], (((1,), (1,)), ((), ())), preferred_element_type=jnp.float32)
        z = jnp.where(ids >= 0, z, -jnp.inf)
        z_ref[:, cols] = z
        hit = jnp.where(ids == label, z, 0.0)
        hit_ref[...] += hit[:, :LANE] + hit[:, LANE:]
        low, high = z[:, :LANE], z[:, LANE:]
        old = top_ref[...]
        top = jnp.maximum(old, jnp.maximum(low, high))
        sum_ref[...] = sum_ref[...] * jnp.exp(old - top) + jnp.exp(low - top) + jnp.exp(high - top)
        top_ref[...] = top
        return carry

    lax.fori_loop(0, tiles, step, 0, unroll=tiles)
    top = jnp.max(top_ref[...], axis=1, keepdims=True)
    total = jnp.sum(sum_ref[...] * jnp.exp(top_ref[...] - top), axis=1, keepdims=True)
    hit = jnp.sum(hit_ref[...], axis=1, keepdims=True)
    lane = lax.broadcasted_iota(jnp.int32, (TOKENS, LANE), 1)
    columns = jnp.where(lane == 0, top, jnp.where(lane == 1, total, jnp.where(lane == 2, hit, 0.0)))
    stat_ref[...] = columns.T[:8]


def grad_kernel(info_ref, ids_ref, z_ref, w_ref, dz_ref, g_ref):
    columns = rows_to_columns(info_ref[...])
    label, log_norm, scale = columns[:, 0:1], columns[:, 1:2], columns[:, 2:3]

    def soft(j, carry):
        cols = pl.ds(pl.multiple_of(j * TILE, TILE), TILE)
        prob = jnp.exp(z_ref[:, cols] - log_norm)
        prob = prob - jnp.where(ids_ref[:, cols] == label, 1.0, 0.0)
        dz_ref[:, cols] = (prob * scale).astype(jnp.bfloat16)
        return carry

    lax.fori_loop(0, w_ref.shape[0] // TILE, soft, 0, unroll=w_ref.shape[0] // TILE)

    def product(j, carry):
        cols = pl.ds(pl.multiple_of(j * TILE, TILE), TILE)
        g_ref[:, cols] = jnp.dot(dz_ref[...], w_ref[:, cols], preferred_element_type=jnp.float32)
        return carry

    lax.fori_loop(0, g_ref.shape[1] // TILE, product, 0, unroll=g_ref.shape[1] // TILE)


def specs(width, columns):
    tokens = lambda size: pl.BlockSpec((TOKENS, size), lambda i: (i, 0))
    info = pl.BlockSpec((8, TOKENS), lambda i: (0, i))
    ids = pl.BlockSpec((1, columns), lambda i: (0, 0))
    weight = pl.BlockSpec((columns, width), lambda i: (0, 0), pipeline_mode=pl.Buffered(1))
    return tokens, info, ids, weight


def logits_call(info, ids, a, w_pair):
    count, width = a.shape
    columns = w_pair.shape[0]
    tokens, info_spec, ids_spec, weight = specs(width, columns)
    return pl.pallas_call(
        logits_kernel,
        grid=(count // TOKENS,),
        in_specs=[info_spec, ids_spec, tokens(width), weight],
        out_specs=[tokens(columns), info_spec],
        out_shape=[jax.ShapeDtypeStruct((count, columns), jnp.float32), jax.ShapeDtypeStruct((8, count), jnp.float32)],
        scratch_shapes=[pltpu.VMEM((TOKENS, LANE), jnp.float32)] * 3,
        compiler_params=pltpu.CompilerParams(vmem_limit_bytes=60 << 20),
        cost_estimate=pl.CostEstimate(
            flops=2 * count * width * columns, bytes_accessed=4 * count * columns + 2 * columns * width, transcendentals=0
        ),
    )(info, ids, a, w_pair)


def grad_call(info, ids, z, w_pair):
    count, columns = z.shape
    width = w_pair.shape[1]
    tokens, info_spec, ids_spec, weight = specs(width, columns)
    return pl.pallas_call(
        grad_kernel,
        grid=(count // TOKENS,),
        in_specs=[info_spec, ids_spec, tokens(columns), weight],
        out_specs=[tokens(columns), tokens(width)],
        out_shape=[jax.ShapeDtypeStruct((count, columns), jnp.bfloat16), jax.ShapeDtypeStruct((count, width), jnp.float32)],
        compiler_params=pltpu.CompilerParams(vmem_limit_bytes=60 << 20),
        cost_estimate=pl.CostEstimate(
            flops=2 * count * width * columns, bytes_accessed=6 * count * columns + 2 * columns * width, transcendentals=0
        ),
    )(info, ids, z, w_pair)


def solution(mesh):
    group_size = mesh.shape["vp"]
    side = math.isqrt(group_size // 2)
    groups = [list(range(core, group_size, 2)) for core in range(2)]
    partner = [(i, i ^ 1) for i in range(group_size)]

    def gather(block):
        return lax.all_gather(block, "vp", axis=0, tiled=True, axis_index_groups=groups)

    def scatter(total):
        return lax.psum_scatter(total, "vp", scatter_dimension=0, tiled=True, axis_index_groups=groups)

    def exchange(value, bits):
        return [value] + [lax.ppermute(value, "vp", [(i, i ^ b) for i in range(group_size)]) for b in bits]

    def merge(stats, bits):
        got = exchange(stats, bits)
        top = got[0][0]
        for other in got[1:]:
            top = jnp.maximum(top, other[0])
        return jnp.stack([top, sum(other[1] * jnp.exp(other[0] - top) for other in got)])

    def group_sum(value):
        for bits in (range(1, 2 * side), range(2 * side, group_size, 2 * side)):
            got = exchange(value, bits)
            while len(got) > 1:
                got = [got[i] + got[i + 1] for i in range(0, len(got), 2)]
            value = got[0]
        return value

    def local_step(hidden, labels, loss_weight, norm_gain, w_local):
        rows, width = hidden.shape
        vocab_local = w_local.shape[1]
        vocab_real = vocab_local * group_size - PAD_COLS
        padded = -(-vocab_local // LANE) * LANE
        me = lax.axis_index("vp")

        x_float = hidden.astype(jnp.float32)
        inv_rms = lax.rsqrt(jnp.mean(x_float * x_float, axis=-1, keepdims=True) + NORM_EPS)
        x_norm = x_float * inv_rms
        normed = (x_norm * norm_gain).astype(jnp.bfloat16)
        ends = [rows * sum(EIGHTHS[:k]) // 8 for k in range(len(EIGHTHS) + 1)]
        a_parts = [gather(normed[lo:hi]) for lo, hi in zip(ends[:-1], ends[1:])]

        both = lax.all_gather(jnp.stack([labels.astype(jnp.float32), loss_weight]), "vp", axis=0)
        weight_sum = jnp.sum(both[:, 1])
        info = both.reshape(group_size // 2, 2, 2, rows)
        info = jnp.where(me % 2 == 0, info[:, 0], info[:, 1])

        w_rows = jnp.pad(w_local.T, ((0, padded - vocab_local), (0, 0)))
        w_pair = jnp.concatenate([w_rows, lax.ppermute(w_rows, "vp", partner)], 0)
        local_ids = jnp.arange(padded)
        ids = jnp.concatenate([me * vocab_local + local_ids, (me ^ 1) * vocab_local + local_ids])
        inside = jnp.concatenate([local_ids, local_ids]) < vocab_local
        ids = jnp.where(inside & (ids < vocab_real), ids, -1).astype(jnp.float32)[None, :]

        loss = jnp.zeros((), jnp.float32)
        d_parts, dz_parts = [], []
        total_g = None
        for part, (lo, hi) in enumerate(zip(ends[:-1], ends[1:])):
            a_c = a_parts[part]
            label = info[:, 0, lo:hi].reshape(1, -1)
            scale = info[:, 1, lo:hi].reshape(1, -1) / weight_sum
            if part:
                a_c, total_g = lax.optimization_barrier((a_c, total_g))
                d_parts.append(scatter(total_g))
            blank = jnp.zeros((7, label.shape[1]), jnp.float32)
            logits, stats = logits_call(jnp.concatenate([label, blank]), ids, a_c, w_pair)
            merged = merge(merge(stats[:2], range(2, 2 * side, 2)), range(2 * side, group_size, 2 * side))
            log_norm = merged[0:1] + jnp.log(merged[1:2])
            loss = loss + jnp.sum(scale * log_norm) / (group_size // 2) - jnp.sum(scale * stats[2:3])
            info_c = jnp.concatenate([label, log_norm, scale, blank[:5]])
            d_logits, total_g = grad_call(info_c, ids, logits, w_pair)
            dz_parts.append(d_logits)
        d_parts.append(scatter(total_g))

        contract = (((0,), (0,)), ((), ()))

        def weight_grad(cols):
            return sum(
                lax.dot_general(dz[:, cols], a, contract, preferred_element_type=jnp.float32) for dz, a in zip(dz_parts, a_parts)
            )

        d_pair = lax.ppermute(weight_grad(slice(padded, None)), "vp", partner)
        d_unembed = (weight_grad(slice(padded)) + d_pair)[:vocab_local].T

        d_normed = jnp.concatenate(d_parts, 0)
        grad_hat = d_normed * norm_gain
        d_input = inv_rms * (grad_hat - x_norm * jnp.mean(grad_hat * x_norm, axis=-1, keepdims=True))
        d_gain = jnp.sum(d_normed * x_norm, axis=0)
        sums = group_sum(jnp.concatenate([d_gain, jnp.full((LANE,), loss)]))
        return sums[width : width + 1], d_input.astype(jnp.bfloat16), d_unembed, sums[:width]

    return jax.shard_map(
        local_step,
        mesh=mesh,
        in_specs=(P(("dp", "vp"), None), P(("dp", "vp")), P(("dp", "vp")), P(None), P(None, "vp")),
        out_specs=(P("dp"), P(("dp", "vp"), None), P("dp", "vp"), P("dp")),
        check_vma=False,
    )
```

```python
import functools
import math

import jax
import jax.numpy as jnp
from jax import lax
from jax.experimental import pallas as pl
from jax.experimental.pallas import tpu as pltpu
from jax.sharding import PartitionSpec as P

NORM_EPS = 1e-5
PAD_COLS = 128
LANE = 128
TILE = 256
TOKENS = 512
EIGHTHS = (4, 4)
LOWEST = float(jnp.finfo(jnp.float32).min)


def rows_to_columns(rows):
    return jnp.concatenate([rows] * (LANE // 8), 0).T


def logits_kernel(info_ref, ids_ref, a_ref, w_ref, z_ref, stat_ref, top_ref, sum_ref, hit_ref):
    label = rows_to_columns(info_ref[...])[:, 0:1]
    top_ref[...] = jnp.full_like(top_ref, LOWEST)
    sum_ref[...] = jnp.zeros_like(sum_ref)
    hit_ref[...] = jnp.zeros_like(hit_ref)
    tiles = w_ref.shape[0] // TILE

    def step(j, carry):
        cols = pl.ds(pl.multiple_of(j * TILE, TILE), TILE)
        ids = ids_ref[:, cols]
        z = lax.dot_general(a_ref[...], w_ref[cols, :], (((1,), (1,)), ((), ())), preferred_element_type=jnp.float32)
        z = jnp.where(ids >= 0, z, -jnp.inf)
        z_ref[:, cols] = z
        hit = jnp.where(ids == label, z, 0.0)
        hit_ref[...] += hit[:, :LANE] + hit[:, LANE:]
        low, high = z[:, :LANE], z[:, LANE:]
        old = top_ref[...]
        top = jnp.maximum(old, jnp.maximum(low, high))
        sum_ref[...] = sum_ref[...] * jnp.exp(old - top) + jnp.exp(low - top) + jnp.exp(high - top)
        top_ref[...] = top
        return carry

    lax.fori_loop(0, tiles, step, 0, unroll=tiles)
    top = jnp.max(top_ref[...], axis=1, keepdims=True)
    total = jnp.sum(sum_ref[...] * jnp.exp(top_ref[...] - top), axis=1, keepdims=True)
    hit = jnp.sum(hit_ref[...], axis=1, keepdims=True)
    lane = lax.broadcasted_iota(jnp.int32, (TOKENS, LANE), 1)
    columns = jnp.where(lane == 0, top, jnp.where(lane == 1, total, jnp.where(lane == 2, hit, 0.0)))
    stat_ref[...] = columns.T[:8]


def grad_kernel(info_ref, ids_ref, z_ref, w_ref, dz_ref, g_ref):
    columns = rows_to_columns(info_ref[...])
    label, log_norm, scale = columns[:, 0:1], columns[:, 1:2], columns[:, 2:3]

    def soft(j, carry):
        cols = pl.ds(pl.multiple_of(j * TILE, TILE), TILE)
        prob = jnp.exp(z_ref[:, cols] - log_norm)
        prob = prob - jnp.where(ids_ref[:, cols] == label, 1.0, 0.0)
        dz_ref[:, cols] = (prob * scale).astype(jnp.bfloat16)
        return carry

    lax.fori_loop(0, w_ref.shape[0] // TILE, soft, 0, unroll=w_ref.shape[0] // TILE)

    def product(j, carry):
        cols = pl.ds(pl.multiple_of(j * TILE, TILE), TILE)
        g_ref[:, cols] = jnp.dot(dz_ref[...], w_ref[:, cols], preferred_element_type=jnp.float32)
        return carry

    lax.fori_loop(0, g_ref.shape[1] // TILE, product, 0, unroll=g_ref.shape[1] // TILE)


def specs(width, columns):
    tokens = lambda size: pl.BlockSpec((TOKENS, size), lambda i: (i, 0))
    info = pl.BlockSpec((8, TOKENS), lambda i: (0, i))
    ids = pl.BlockSpec((1, columns), lambda i: (0, 0))
    weight = pl.BlockSpec((columns, width), lambda i: (0, 0), pipeline_mode=pl.Buffered(1))
    return tokens, info, ids, weight


def logits_call(info, ids, a, w_pair):
    count, width = a.shape
    columns = w_pair.shape[0]
    tokens, info_spec, ids_spec, weight = specs(width, columns)
    return pl.pallas_call(
        logits_kernel,
        grid=(count // TOKENS,),
        in_specs=[info_spec, ids_spec, tokens(width), weight],
        out_specs=[tokens(columns), info_spec],
        out_shape=[jax.ShapeDtypeStruct((count, columns), jnp.float32), jax.ShapeDtypeStruct((8, count), jnp.float32)],
        scratch_shapes=[pltpu.VMEM((TOKENS, LANE), jnp.float32)] * 3,
        compiler_params=pltpu.CompilerParams(vmem_limit_bytes=60 << 20),
        cost_estimate=pl.CostEstimate(
            flops=2 * count * width * columns, bytes_accessed=4 * count * columns + 2 * columns * width, transcendentals=0
        ),
    )(info, ids, a, w_pair)


def grad_call(info, ids, z, w_pair):
    count, columns = z.shape
    width = w_pair.shape[1]
    tokens, info_spec, ids_spec, weight = specs(width, columns)
    return pl.pallas_call(
        grad_kernel,
        grid=(count // TOKENS,),
        in_specs=[info_spec, ids_spec, tokens(columns), weight],
        out_specs=[tokens(columns), tokens(width)],
        out_shape=[jax.ShapeDtypeStruct((count, columns), jnp.bfloat16), jax.ShapeDtypeStruct((count, width), jnp.float32)],
        compiler_params=pltpu.CompilerParams(vmem_limit_bytes=60 << 20),
        cost_estimate=pl.CostEstimate(
            flops=2 * count * width * columns, bytes_accessed=6 * count * columns + 2 * columns * width, transcendentals=0
        ),
    )(info, ids, z, w_pair)


def solution(mesh):
    group_size = mesh.shape["vp"]
    side = math.isqrt(group_size // 2)
    groups = [list(range(core, group_size, 2)) for core in range(2)]
    partner = [(i, i ^ 1) for i in range(group_size)]

    def gather(block):
        return lax.all_gather(block, "vp", axis=0, tiled=True, axis_index_groups=groups)

    def scatter(total):
        return lax.psum_scatter(total, "vp", scatter_dimension=0, tiled=True, axis_index_groups=groups)

    def exchange(value, bits):
        return [value] + [lax.ppermute(value, "vp", [(i, i ^ b) for i in range(group_size)]) for b in bits]

    def merge(stats, bits):
        got = exchange(stats, bits)
        top = got[0][0]
        for other in got[1:]:
            top = jnp.maximum(top, other[0])
        return jnp.stack([top, sum(other[1] * jnp.exp(other[0] - top) for other in got)])

    def group_sum(value):
        for bits in (range(1, 2 * side), range(2 * side, group_size, 2 * side)):
            got = exchange(value, bits)
            while len(got) > 1:
                got = [got[i] + got[i + 1] for i in range(0, len(got), 2)]
            value = got[0]
        return value

    def local_step(hidden, labels, loss_weight, norm_gain, w_local):
        rows, width = hidden.shape
        vocab_local = w_local.shape[1]
        vocab_real = vocab_local * group_size - PAD_COLS
        padded = -(-vocab_local // LANE) * LANE
        me = lax.axis_index("vp")

        x_float = hidden.astype(jnp.float32)
        inv_rms = lax.rsqrt(jnp.mean(x_float * x_float, axis=-1, keepdims=True) + NORM_EPS)
        x_norm = x_float * inv_rms
        normed = (x_norm * norm_gain).astype(jnp.bfloat16)
        ends = [rows * sum(EIGHTHS[:k]) // 8 for k in range(len(EIGHTHS) + 1)]
        a_parts = [gather(normed[lo:hi]) for lo, hi in zip(ends[:-1], ends[1:])]

        both = lax.all_gather(jnp.stack([labels.astype(jnp.float32), loss_weight]), "vp", axis=0)
        weight_sum = jnp.sum(both[:, 1])
        info = both.reshape(group_size // 2, 2, 2, rows)
        info = jnp.where(me % 2 == 0, info[:, 0], info[:, 1])

        w_rows = jnp.pad(w_local.T, ((0, padded - vocab_local), (0, 0)))
        w_pair = jnp.concatenate([w_rows, lax.ppermute(w_rows, "vp", partner)], 0)
        local_ids = jnp.arange(padded)
        ids = jnp.concatenate([me * vocab_local + local_ids, (me ^ 1) * vocab_local + local_ids])
        inside = jnp.concatenate([local_ids, local_ids]) < vocab_local
        ids = jnp.where(inside & (ids < vocab_real), ids, -1).astype(jnp.float32)[None, :]

        d_parts, dz_parts, loss_parts = [], [], []
        total_g = None
        for part, (lo, hi) in enumerate(zip(ends[:-1], ends[1:])):
            a_c = a_parts[part]
            label = info[:, 0, lo:hi].reshape(1, -1)
            scale = info[:, 1, lo:hi].reshape(1, -1) / weight_sum
            if part:
                a_c, total_g = lax.optimization_barrier((a_c, total_g))
                d_parts.append(scatter(total_g))
            blank = jnp.zeros((7, label.shape[1]), jnp.float32)
            logits, stats = logits_call(jnp.concatenate([label, blank]), ids, a_c, w_pair)
            merged = merge(merge(stats[:2], range(2, 2 * side, 2)), range(2 * side, group_size, 2 * side))
            log_norm = merged[0:1] + jnp.log(merged[1:2])
            loss_parts.append((scale, log_norm, stats))
            info_c = jnp.concatenate([label, log_norm, scale, blank[:5]])
            d_logits, total_g = grad_call(info_c, ids, logits, w_pair)
            dz_parts.append(d_logits)
        loss_parts, total_g = lax.optimization_barrier((loss_parts, total_g))
        d_parts.append(scatter(total_g))
        loss = jnp.zeros((), jnp.float32)
        for scale, log_norm, stats in loss_parts:
            loss = loss + jnp.sum(scale * log_norm) / (group_size // 2) - jnp.sum(scale * stats[2:3])

        contract = (((0,), (0,)), ((), ()))

        def weight_grad(cols):
            return sum(
                lax.dot_general(dz[:, cols], a, contract, preferred_element_type=jnp.float32) for dz, a in zip(dz_parts, a_parts)
            )

        d_pair = lax.ppermute(weight_grad(slice(padded, None)), "vp", partner)
        d_unembed = (weight_grad(slice(padded)) + d_pair)[:vocab_local].T

        d_inputs, d_gain = [], 0.0
        for d_normed, lo, hi in zip(d_parts, ends[:-1], ends[1:]):
            x_part = x_norm[lo:hi]
            grad_hat = d_normed * norm_gain
            d_input = inv_rms[lo:hi] * (grad_hat - x_part * jnp.mean(grad_hat * x_part, axis=-1, keepdims=True))
            d_inputs.append(d_input.astype(jnp.bfloat16))
            d_gain = d_gain + jnp.sum(d_normed * x_part, axis=0)
        sums = group_sum(jnp.concatenate([d_gain, jnp.full((LANE,), loss)]))
        return sums[width : width + 1], jnp.concatenate(d_inputs, 0), d_unembed, sums[:width]

    return jax.shard_map(
        local_step,
        mesh=mesh,
        in_specs=(P(("dp", "vp"), None), P(("dp", "vp")), P(("dp", "vp")), P(None), P(None, "vp")),
        out_specs=(P("dp"), P(("dp", "vp"), None), P("dp", "vp"), P("dp")),
        check_vma=False,
    )
```
